32 devices in a mesh: site: 8 (over z, x), dom: 4 (over y, core).
Axes of the slice: x: 2, y: 2, z: 4, core: 2. Of those that a mesh axis runs over, the one named last changes fastest.
Arguments:
- top_partial: float32 [16, 61, 4, 8192], P(None, None, 'dom', 'site'), may hold values from 0.001 to 1
- bottom_partial: float32 [16, 61, 4, 8192], P(None, None, 'dom', 'site'), may hold values from 0.001 to 1
- left_vectors: float32 [256, 61, 61], P('dom'), may hold values from 0.05 to 1
- right_vectors: float32 [256, 61, 61], P('dom'), may hold values from 0.05 to 1
- decay_rates: float32 [256, 61], P('dom'), may hold values from 0.05 to 8
- state_weights: float32 [256, 61], P('dom'), may hold values from 0.002 to 0.05
- part_rates: float32 [256], P('dom'), may hold values from 0.3 to 3
- branch_lengths: float32 [1997], replicated, may hold values from 0.02 to 0.5
- pattern_weights: int32 [4, 8192], P('dom', 'site'), may hold values from 0 to 9
- block_partition: int32 [4, 64], P('dom', 'site'), may hold values from 0 to 255
- chosen_branches: int32 [16], replicated, may hold values from 0 to 1996, as said below
Outputs:
- site_loglik: float32 [16, 4, 8192], P(None, 'dom', 'site')
- part_derivs: float32 [2, 16, 256], P(None, None, 'dom')
- new_lengths: float32 [1997], replicated
The draws below stay inside these ranges and needn't reach their ends.
Inputs may be any that keep to these rules, and one draw needn't show every extreme that they name: `chosen_branches`: distinct branch numbers.
All inputs are finite; a program needn't handle non-finite values.
Results may differ from the reference program's by a relative error of at most 0.0003.
Values sent between devices are 32-bit elements; how exact they have to be, the bound alone decides.
A program may use at most 64 MiB of HBM per device.

```python
import math
import jax
import jax.numpy as jnp
import numpy as np
from jax import lax

STATES = 61
BR = 16
BLK = 128
TREE_BR = 1997
PARTS_SIZE = 256
SG = 8192
NBLK_G = 64
N_DOM = 4


def draw_chosen_branches(key, part):
    picked = jax.random.permutation(jax.random.fold_in(key, 17), TREE_BR)
    return picked[:BR].astype(jnp.int32)


def with_ends(result, key, low, top_value):
    spot = [jax.random.randint(jax.random.fold_in(key, axis), (), 0, length) for axis, length in enumerate(result.shape)]
    longest = result.shape.index(max(result.shape))
    next_to = spot[:longest] + [(spot[longest] + 1) % result.shape[longest]] + spot[longest + 1:]
    return result.at[tuple(spot)].set(low).at[tuple(next_to)].set(top_value)


def block_levels(own_key, dims, shards, least, high):
    def one(position, parts):
        draws = jax.random.uniform(jax.random.fold_in(jax.random.fold_in(own_key, 6), position), (parts,), jnp.float32, least / len(shards), high / len(shards))
        return jnp.repeat(jnp.exp(draws), dims[position] // parts).reshape((-1,) + (1,) * (len(dims) - position - 1))

    level = one(*shards[0])
    for cut in shards[1:]:
        level = level * one(*cut)
    return level


def cumulative_ranks(count, skew):
    loads = [(1 << 20) // math.isqrt(standing ** skew) + 1 for standing in range(1, count + 1)]
    scale = 1 + sum(loads) // (1 << 30)
    return np.cumsum(np.array([max(1, weight // scale) for weight in loads]))


def ranked(key, extent, amount, slope):
    grid = cumulative_ranks(amount, slope)
    ticket = jax.random.randint(jax.random.fold_in(key, 1), extent, 0, int(grid[amount - 1]))
    standing = jnp.searchsorted(jnp.asarray(grid, jnp.int32), ticket, side="right")
    return jax.random.permutation(jax.random.fold_in(key, 2), amount)[standing].astype(jnp.int32)


def setup_inputs(seed: int = 0) -> dict:
    splits = jax.random.split(jax.random.key(seed), 12)
    top_partial = jnp.clip(jnp.exp(math.log(1.0) - 6.9077552 * jax.random.uniform(splits[0], (BR, STATES, N_DOM, SG), jnp.float32) ** block_levels(splits[0], (BR, STATES, N_DOM, SG), ((2, 4), (3, 8)), -0.2, 0.2)), 0.001, 1.0)
    bottom_partial = jnp.clip(jnp.exp(math.log(1.0) - 6.9077552 * jax.random.uniform(splits[1], (BR, STATES, N_DOM, SG), jnp.float32) ** block_levels(splits[1], (BR, STATES, N_DOM, SG), ((2, 4), (3, 8)), -0.2, 0.2)), 0.001, 1.0)
    left_vectors = jnp.clip(0.05 + 0.95 * jax.random.uniform(splits[2], (PARTS_SIZE, STATES, STATES), jnp.float32) ** block_levels(splits[2], (PARTS_SIZE, STATES, STATES), ((0, 4),), -0.2, 0.2), 0.05, 1.0)
    right_vectors = jnp.clip(0.05 + 0.95 * jax.random.uniform(splits[3], (PARTS_SIZE, STATES, STATES), jnp.float32) ** block_levels(splits[3], (PARTS_SIZE, STATES, STATES), ((0, 4),), -0.2, 0.2), 0.05, 1.0)
    decay_rates = jnp.clip(jnp.exp(math.log(8.0) - 5.075174 * jax.random.uniform(splits[4], (PARTS_SIZE, STATES), jnp.float32) ** block_levels(splits[4], (PARTS_SIZE, STATES), ((0, 4),), -0.2, 0.2)), 0.05, 8.0)
    state_weights = jnp.clip(jnp.exp(math.log(0.05) - 3.218876 * jax.random.uniform(splits[5], (PARTS_SIZE, STATES), jnp.float32) ** block_levels(splits[5], (PARTS_SIZE, STATES), ((0, 4),), -0.2, 0.2)), 0.002, 0.05)
    part_rates = jnp.clip(jnp.exp(math.log(3.0) - 2.3025851 * jax.random.uniform(splits[6], (PARTS_SIZE,), jnp.float32) ** block_levels(splits[6], (PARTS_SIZE,), ((0, 4),), -0.2, 0.2)), 0.3, 3.0)
    branch_lengths = jnp.clip(jnp.exp(jax.random.uniform(splits[7], (TREE_BR,), jnp.float32, math.log(0.02), math.log(0.5))), 0.02, 0.5)
    pattern_weights = with_ends(jax.random.randint(splits[8], (N_DOM, SG), 0, 10), jax.random.fold_in(splits[8], 1), 0, 9).astype(jnp.int32)
    block_partition = with_ends(ranked(splits[9], (N_DOM, NBLK_G), PARTS_SIZE, 2), jax.random.fold_in(splits[9], 3), 0, PARTS_SIZE - 1).astype(jnp.int32)
    chosen_branches = draw_chosen_branches(jax.random.fold_in(splits[11], 71), 0)
    return {"top_partial": top_partial, "bottom_partial": bottom_partial, "left_vectors": left_vectors, "right_vectors": right_vectors, "decay_rates": decay_rates, "state_weights": state_weights, "part_rates": part_rates, "branch_lengths": branch_lengths, "pattern_weights": pattern_weights, "block_partition": block_partition, "chosen_branches": chosen_branches}


def project(upper, lower, vec_left, vec_right, state_w):
    scaled = upper * jnp.transpose(state_w)[None, :, :, None]
    lefts = jnp.einsum('binl,nik->bknl', scaled, vec_left, precision=lax.Precision.HIGHEST)
    rights = jnp.einsum('nkj,bjnl->bknl', vec_right, lower, precision=lax.Precision.HIGHEST)
    return lefts, rights


def finish(lefts, rights, exponent, times, weight_f):
    joint = lefts * rights
    expo = jnp.transpose(exponent)[None, :, :, None]
    decayed = joint * jnp.exp(expo * times[:, None, None, None])
    like_zero = jnp.sum(decayed, axis=1)
    like_one = jnp.sum(decayed * expo, axis=1)
    like_two = jnp.sum(decayed * expo * expo, axis=1)
    first = like_one / like_zero
    second = like_two / like_zero - first * first
    loglik = weight_f[None] * jnp.log(like_zero)
    sums = jnp.stack([jnp.sum(weight_f[None] * first, axis=-1), jnp.sum(weight_f[None] * second, axis=-1)])
    return loglik, sums


def reference(top_partial, bottom_partial, left_vectors, right_vectors, decay_rates, state_weights, part_rates, branch_lengths, pattern_weights, block_partition, chosen_branches):
    times = branch_lengths[chosen_branches]
    upper_all = jnp.moveaxis(top_partial, 2, 0)
    lower_all = jnp.moveaxis(bottom_partial, 2, 0)

    def one_group(items):
        upper, lower, weights_g, blocks = items
        nblocks = blocks.shape[0]
        upper = upper.reshape(BR, STATES, nblocks, BLK)
        lower = lower.reshape(BR, STATES, nblocks, BLK)
        vec_left = left_vectors[blocks]
        vec_right = right_vectors[blocks]
        exponent = -decay_rates[blocks] * part_rates[blocks][:, None]
        lefts, rights = project(upper, lower, vec_left, vec_right, state_weights[blocks])
        weight_f = weights_g.astype(jnp.float32).reshape(nblocks, BLK)
        loglik, sums = finish(lefts, rights, exponent, times, weight_f)
        onehot = (blocks[:, None] == jnp.arange(PARTS_SIZE, dtype=jnp.int32)[None, :]).astype(jnp.float32)
        part_sums = jnp.einsum('abn,np->abp', sums, onehot, precision=lax.Precision.HIGHEST)
        return loglik.reshape(BR, nblocks * BLK), part_sums

    logliks, part_all = lax.map(one_group, (upper_all, lower_all, pattern_weights, block_partition))
    site_loglik = jnp.moveaxis(logliks, 0, 1)
    part_derivs = jnp.sum(part_all, axis=0)
    totals = jnp.sum(part_derivs, axis=2)
    updated = times - totals[0] / totals[1]
    new_lengths = branch_lengths.at[chosen_branches].set(updated)
    return site_loglik, part_derivs, new_lengths
```

```python
import functools

import jax
import jax.numpy as jnp
from jax import lax
from jax.experimental import pallas as pl
from jax.experimental.pallas import tpu as pltpu
from jax.sharding import PartitionSpec as P

BLK = 128
MESH = pl.DeviceIdType.MESH
F32 = jnp.float32
BF16 = jnp.bfloat16


def round_up(value, unit):
    return (value + unit - 1) // unit * unit


def split(value):
    high = value.astype(BF16)
    return high, (value - high.astype(F32)).astype(BF16)


def body(
    cfg,
    top_hbm, bottom_hbm, left_hbm, right_hbm,
    decay_ref, weight_ref, rate_s, lengths_s, chosen_s, lengths_ref,
    pattern_ref, blocks_s, blocks_ref,
    loglik_ref, share_ref, new_ref,
    top_v, bottom_v, left_v, right_v, req_v, req_s, mine, passed, got,
    top_x, bottom_x, like_v, acc, dom_in, site_out, site_in,
    load_sem, req_send, req_recv, req_local, tab_send, tab_recv,
    dom_send, dom_recv, site_send, site_recv,
):
    doms, sites, branches, states, nblk, owned, pad, chunk = cfg
    me = lax.axis_index("dom")
    spot = lax.axis_index("site")
    dom_bits = doms.bit_length() - 1
    site_bits = sites.bit_length() - 1
    nchunk = nblk // chunk
    used = branches * states * nblk

    loads = [
        pltpu.make_async_copy(left_hbm, left_v, load_sem.at[0]),
        pltpu.make_async_copy(right_hbm, right_v, load_sem.at[1]),
        pltpu.make_async_copy(top_hbm, top_v.at[pl.ds(0, used)], load_sem.at[2]),
        pltpu.make_async_copy(bottom_hbm, bottom_v.at[pl.ds(0, used)], load_sem.at[3]),
    ]
    for load in loads:
        load.start()

    barrier = pltpu.get_barrier_semaphore()
    for delta in range(1, doms):
        pl.semaphore_signal(
            barrier, inc=1, device_id={"dom": me ^ delta}, device_id_type=MESH
        )
    for bit in range(site_bits):
        pl.semaphore_signal(
            barrier, inc=1, device_id={"site": spot ^ (1 << bit)}, device_id_type=MESH
        )

    req_v[0] = jnp.zeros((1, BLK), jnp.int32)
    req_v[0, 0:1, 0:nblk] = blocks_ref[...]
    tail = top_v.shape[0] - used
    top_v[pl.ds(used, tail), :] = jnp.zeros((tail, BLK), F32)
    bottom_v[pl.ds(used, tail), :] = jnp.zeros((tail, BLK), F32)
    mine[...] = jnp.zeros(mine.shape, F32)

    pl.semaphore_wait(barrier, doms - 1 + site_bits)

    asks = []
    for delta in range(1, doms):
        ask = pltpu.make_async_remote_copy(
            src_ref=req_v.at[0],
            dst_ref=req_v.at[delta],
            send_sem=req_send.at[delta],
            recv_sem=req_recv.at[delta],
            device_id={"dom": me ^ delta},
            device_id_type=MESH,
        )
        ask.start()
        asks.append(ask)
    loads[0].wait()
    loads[1].wait()
    for ask in asks:
        ask.wait()
    local = pltpu.make_async_copy(req_v, req_s, req_local)
    local.start()
    local.wait()

    def gather(delta):
        def step(n, carry):
            relative = req_s[delta, 0, n] - me * owned
            inside = jnp.logical_and(relative >= 0, relative < owned)
            keep = jnp.where(inside, 1.0, 0.0).astype(F32)
            p = jnp.clip(relative, 0, owned - 1)
            mine[delta, n, 0:states, 0:states] = left_v[p] * keep
            mine[delta, n, 0:states, pad:pad + states] = right_v[p] * keep
            rate = rate_s[p] * keep
            mine[delta, n, states:states + 1, pad:pad + states] = -decay_ref[pl.ds(p, 1), :] * rate
            mine[delta, n, states + 1:states + 2, pad:pad + states] = (
                weight_ref[pl.ds(p, 1), :] * keep
            )
            return carry

        lax.fori_loop(0, nblk, step, 0)

    def convert(n, carry):
        for source, dest in ((top_v, top_x), (bottom_v, bottom_x)):
            for b in range(branches):
                rows = source[pl.ds(b * states * nblk + n, pad, stride=nblk), :]
                high, low = split(rows)
                at = n * (branches // 2) + b // 2
                lanes = (b % 2) * BLK
                dest[at, 0:pad, lanes:lanes + BLK] = high
                dest[at, pad:2 * pad, lanes:lanes + BLK] = low
        return carry

    sends = {}
    for bit in range(dom_bits):
        moves = [d for d in range(doms) if d % (1 << bit) == 0 and (d >> bit) & 1]
        for d in sorted(moves, reverse=True):
            to = d ^ (1 << bit)
            for c in range(nchunk):
                at = pl.ds(c * chunk, chunk)
                sends[(bit, d, c)] = pltpu.make_async_remote_copy(
                    src_ref=(mine if bit == 0 else passed).at[d, at],
                    dst_ref=got.at[bit, to, at],
                    send_sem=tab_send.at[bit, d, c],
                    recv_sem=tab_recv.at[bit, to, c],
                    device_id={"dom": me ^ (1 << bit)},
                    device_id_type=MESH,
                )

    first = [d for d in range(doms) if d & 1]
    for d in sorted(first, reverse=True):
        gather(d)
        for c in range(nchunk):
            sends[(0, d, c)].start()
    for d in sorted((d for d in range(doms) if not d & 1), reverse=True):
        gather(d)
    loads[2].wait()
    loads[3].wait()
    lax.fori_loop(0, nblk // 2, convert, 0)
    for bit in range(1, dom_bits):
        moves = [d for d in range(doms) if d % (1 << bit) == 0 and (d >> bit) & 1]
        for d in sorted(moves, reverse=True):
            for c in range(nchunk):
                at = pl.ds(c * chunk, chunk)
                total = mine[d, at]
                for earlier in range(bit):
                    sends[(earlier, d | (1 << earlier), c)].wait_recv()
                    total = total + got[earlier, d, at]
                passed[d, at] = total
                sends[(bit, d, c)].start()
    lax.fori_loop(nblk // 2, nblk, convert, 0)

    acc[...] = jnp.zeros(acc.shape, F32)
    lane = lax.broadcasted_iota(jnp.int32, (2 * branches, BLK), 1)
    times = [lengths_s[chosen_s[b]] for b in range(branches)]

    def block(n, carry):
        tile = mine[0, n]
        for bit in range(dom_bits):
            tile = tile + got[bit, 0, n]
        turned = jnp.transpose(tile)
        w_row = tile[states + 1:states + 2, pad:2 * pad]
        l_high, l_low = split(turned[0:pad, :] * w_row)
        r_high, r_low = split(tile[:, pad:2 * pad])
        l_all = jnp.concatenate([l_high, l_high, l_low], axis=1)
        r_all = jnp.concatenate([r_high, r_high, r_low], axis=1)
        expo = jnp.broadcast_to(turned[pad:2 * pad, states:states + 1], (pad, BLK))
        for half in range(branches // 2):
            at = n * (branches // 2) + half
            t_x = top_x[at]
            b_x = bottom_x[at]
            lefts = jnp.dot(
                l_all, jnp.concatenate([t_x, t_x[0:pad]], axis=0), preferred_element_type=F32
            )
            rights = jnp.dot(
                r_all, jnp.concatenate([b_x, b_x[0:pad]], axis=0), preferred_element_type=F32
            )
            joint = lefts * rights
            for side in range(2):
                b = 2 * half + side
                decayed = joint[:, side * BLK:(side + 1) * BLK] * jnp.exp(expo * times[b])
                once = decayed * expo
                twice = once * expo
                like_v[0, b:b + 1, :] = jnp.sum(decayed, axis=0, keepdims=True)
                like_v[1, b:b + 1, :] = jnp.sum(once, axis=0, keepdims=True)
                like_v[2, b:b + 1, :] = jnp.sum(twice, axis=0, keepdims=True)
        like0 = like_v[0]
        first_d = like_v[1] / like0
        second_d = like_v[2] / like0 - first_d * first_d
        w_sites = pattern_ref[pl.ds(n, 1), :].astype(F32)
        loglik_ref[pl.ds(n, branches, stride=nblk), :] = w_sites * jnp.log(like0)
        both = jnp.concatenate([first_d, second_d], axis=0) * w_sites
        sums = jnp.sum(both, axis=1, keepdims=True)
        p = blocks_s[0, n]
        for d in range(doms):
            hit = jnp.logical_and(lane + d * owned == p, lane < owned)
            hit = jnp.logical_or(hit, lane == owned)
            acc[d] = acc[d] + jnp.where(hit, sums, 0.0)
        return carry

    for c in range(nchunk):
        for bit in range(dom_bits):
            sends[(bit, 1 << bit, c)].wait_recv()
        lax.fori_loop(c * chunk, (c + 1) * chunk, block, 0)

    scatter = []
    for delta in range(1, doms):
        copy = pltpu.make_async_remote_copy(
            src_ref=acc.at[me ^ delta],
            dst_ref=dom_in.at[me],
            send_sem=dom_send.at[delta],
            recv_sem=dom_recv.at[delta],
            device_id={"dom": me ^ delta},
            device_id_type=MESH,
        )
        copy.start()
        scatter.append(copy)
    dom_in[me] = acc[me]
    for copy in scatter:
        copy.wait_recv()
    total = dom_in[0]
    for d in range(1, doms):
        total = total + dom_in[d]
    pending = []
    for bit in range(site_bits):
        site_out[bit] = total
        copy = pltpu.make_async_remote_copy(
            src_ref=site_out.at[bit],
            dst_ref=site_in.at[bit],
            send_sem=site_send.at[bit],
            recv_sem=site_recv.at[bit],
            device_id={"site": spot ^ (1 << bit)},
            device_id_type=MESH,
        )
        copy.start()
        pending.append(copy)
        copy.wait_recv()
        total = total + site_in[bit]

    share_ref[...] = total[:, 0:owned]
    sums = total[:, owned:owned + 1]
    ratio = sums[0:branches] / sums[branches:2 * branches]
    new = lengths_ref[...]
    place = lax.broadcasted_iota(jnp.int32, new.shape, 1)
    for b in range(branches):
        value = times[b] - ratio[b:b + 1, :]
        new = jnp.where(place == chosen_s[b], value, new)
    new_ref[...] = new

    for copy in scatter + pending:
        copy.wait_send()
    for copy in sends.values():
        copy.wait_send()


def on_device(
    top_partial,
    bottom_partial,
    left_vectors,
    right_vectors,
    decay_rates,
    state_weights,
    part_rates,
    branch_lengths,
    pattern_weights,
    block_partition,
    chosen_branches,
):
    doms = lax.axis_size("dom")
    sites = lax.axis_size("site")
    branches, states, _, sites_here = top_partial.shape
    nblk = sites_here // BLK
    owned = left_vectors.shape[0]
    tree = branch_lengths.shape[0]
    pad = round_up(states + 2, 64)
    chunk = 2 if nblk % 2 == 0 else 1
    nchunk = nblk // chunk
    dom_bits = doms.bit_length() - 1
    site_bits = sites.bit_length() - 1
    used = branches * states * nblk
    room = used + (pad - states) * nblk
    cfg = (doms, sites, branches, states, nblk, owned, pad, chunk)
    hbm = pl.BlockSpec(memory_space=pl.ANY)
    vmem = pl.BlockSpec(memory_space=pltpu.VMEM)
    smem = pl.BlockSpec(memory_space=pltpu.SMEM)
    tile = (pad, 2 * pad)
    dma = pltpu.SemaphoreType.DMA
    loglik, share, new = pl.pallas_call(
        functools.partial(body, cfg),
        out_shape=(
            jax.ShapeDtypeStruct((branches * nblk, BLK), F32),
            jax.ShapeDtypeStruct((2 * branches, owned), F32),
            jax.ShapeDtypeStruct((1, tree), F32),
        ),
        in_specs=[hbm, hbm, hbm, hbm, vmem, vmem, smem, smem, smem, vmem, vmem, smem, vmem],
        out_specs=(vmem, vmem, vmem),
        scratch_shapes=[
            pltpu.VMEM((room, BLK), F32),
            pltpu.VMEM((room, BLK), F32),
            pltpu.VMEM((owned, states, states), F32),
            pltpu.VMEM((owned, states, states), F32),
            pltpu.VMEM((doms, 1, BLK), jnp.int32),
            pltpu.SMEM((doms, 1, BLK), jnp.int32),
            pltpu.VMEM((doms, nblk) + tile, F32),
            pltpu.VMEM((doms, nblk) + tile, F32),
            pltpu.VMEM((dom_bits, doms, nblk) + tile, F32),
            pltpu.VMEM((nblk * branches // 2, 2 * pad, 2 * BLK), BF16),
            pltpu.VMEM((nblk * branches // 2, 2 * pad, 2 * BLK), BF16),
            pltpu.VMEM((3, branches, BLK), F32),
            pltpu.VMEM((doms, 2 * branches, BLK), F32),
            pltpu.VMEM((doms, 2 * branches, BLK), F32),
            pltpu.VMEM((site_bits, 2 * branches, BLK), F32),
            pltpu.VMEM((site_bits, 2 * branches, BLK), F32),
            dma((4,)),
            dma((doms,)),
            dma((doms,)),
            dma,
            dma((dom_bits, doms, nchunk)),
            dma((dom_bits, doms, nchunk)),
            dma((doms,)),
            dma((doms,)),
            dma((site_bits,)),
            dma((site_bits,)),
        ],
        compiler_params=pltpu.CompilerParams(
            collective_id=0, has_side_effects=True, vmem_limit_bytes=56 * 1024 * 1024
        ),
    )(
        top_partial.reshape(used, BLK),
        bottom_partial.reshape(used, BLK),
        left_vectors,
        right_vectors,
        decay_rates,
        state_weights,
        part_rates,
        branch_lengths,
        chosen_branches,
        branch_lengths.reshape(1, tree),
        pattern_weights.reshape(nblk, BLK),
        block_partition,
        block_partition,
    )
    return (
        loglik.reshape(branches, 1, sites_here),
        share.reshape(2, branches, owned),
        new.reshape(tree),
    )


def solution(mesh):
    return jax.shard_map(
        on_device,
        mesh=mesh,
        in_specs=(
            P(None, None, "dom", "site"),
            P(None, None, "dom", "site"),
            P("dom", None, None),
            P("dom", None, None),
            P("dom", None),
            P("dom", None),
            P("dom"),
            P(),
            P("dom", "site"),
            P("dom", "site"),
            P(),
        ),
        out_specs=(P(None, "dom", "site"), P(None, None, "dom"), P()),
        check_vma=False,
    )
```

```python
import functools

import jax
import jax.numpy as jnp
from jax import lax
from jax.experimental import pallas as pl
from jax.experimental.pallas import tpu as pltpu
from jax.sharding import PartitionSpec as P

BLK = 128
MESH = pl.DeviceIdType.MESH
F32 = jnp.float32
BF16 = jnp.bfloat16


def round_up(value, unit):
    return (value + unit - 1) // unit * unit


def split(value):
    high = value.astype(BF16)
    return high, (value - high.astype(F32)).astype(BF16)


def body(
    cfg,
    top_hbm, bottom_hbm, left_hbm, right_hbm,
    decay_ref, weight_ref, rate_s, lengths_s, chosen_s,
    pattern_ref, blocks_s, blocks_ref,
    like_ref, final_ref,
    top_v, bottom_v, left_v, right_v, req_v, req_s, mine, passed, got,
    top_x, bottom_x, like_v, acc, dom_in, site_out, site_in,
    load_sem, req_send, req_recv, req_local, tab_send, tab_recv,
    dom_send, dom_recv, site_send, site_recv,
):
    doms, sites, inner, branches, states, nblk, owned, pad, chunk = cfg
    me = lax.axis_index("dom")
    spot = lax.axis_index("site")
    dom_bits = doms.bit_length() - 1
    outer = sites // inner
    near, far = lax.rem(spot, inner), spot // inner
    nchunk = nblk // chunk
    used = branches * states * nblk

    plane = [(d, x) for d in range(doms) for x in range(inner) if d or x]

    def in_plane(d, x):
        return {"dom": me ^ d, "site": far * inner + lax.rem(near + x, inner)}

    def in_line(k):
        return {"site": lax.rem(far + k, outer) * inner + near}

    loads = [
        pltpu.make_async_copy(left_hbm, left_v, load_sem.at[0]),
        pltpu.make_async_copy(right_hbm, right_v, load_sem.at[1]),
        pltpu.make_async_copy(top_hbm, top_v.at[pl.ds(0, used)], load_sem.at[2]),
        pltpu.make_async_copy(bottom_hbm, bottom_v.at[pl.ds(0, used)], load_sem.at[3]),
    ]
    for load in loads:
        load.start()

    barrier = pltpu.get_barrier_semaphore()
    for d, x in plane:
        pl.semaphore_signal(barrier, inc=1, device_id=in_plane(d, x), device_id_type=MESH)
    for k in range(1, outer):
        pl.semaphore_signal(barrier, inc=1, device_id=in_line(k), device_id_type=MESH)

    req_v[0] = jnp.zeros((1, BLK), jnp.int32)
    req_v[0, 0:1, 0:nblk] = blocks_ref[...]
    tail = top_v.shape[0] - used
    top_v[pl.ds(used, tail), :] = jnp.zeros((tail, BLK), F32)
    bottom_v[pl.ds(used, tail), :] = jnp.zeros((tail, BLK), F32)
    mine[...] = jnp.zeros(mine.shape, F32)

    pl.semaphore_wait(barrier, len(plane) + outer - 1)

    asks = []
    for delta in range(1, doms):
        ask = pltpu.make_async_remote_copy(
            src_ref=req_v.at[0],
            dst_ref=req_v.at[delta],
            send_sem=req_send.at[delta],
            recv_sem=req_recv.at[delta],
            device_id={"dom": me ^ delta},
            device_id_type=MESH,
        )
        ask.start()
        asks.append(ask)
    loads[0].wait()
    loads[1].wait()
    for ask in asks:
        ask.wait()
    local = pltpu.make_async_copy(req_v, req_s, req_local)
    local.start()
    local.wait()

    def gather(delta, c=None):
        def step(n, carry):
            relative = req_s[delta, 0, n] - me * owned
            inside = jnp.logical_and(relative >= 0, relative < owned)
            keep = jnp.where(inside, 1.0, 0.0).astype(F32)
            p = jnp.clip(relative, 0, owned - 1)
            mine[delta, n, 0:states, 0:states] = left_v[pl.ds(p, states, stride=owned), :] * keep
            mine[delta, n, 0:states, pad:pad + states] = right_v[pl.ds(p, states, stride=owned), :] * keep
            rate = rate_s[p] * keep
            mine[delta, n, states:states + 1, pad:pad + states] = -decay_ref[pl.ds(p, 1), :] * rate
            mine[delta, n, states + 1:states + 2, pad:pad + states] = (
                weight_ref[pl.ds(p, 1), :] * keep
            )
            return carry

        if c is None:
            lax.fori_loop(0, nblk, step, 0)
        else:
            lax.fori_loop(c * chunk, (c + 1) * chunk, step, 0)

    def convert(n, carry):
        for source, dest in ((top_v, top_x), (bottom_v, bottom_x)):
            for b in range(branches):
                rows = source[pl.ds(b * states * nblk + n, pad, stride=nblk), :]
                high, low = split(rows)
                at = n * (branches // 2) + b // 2
                lanes = (b % 2) * BLK
                dest[at, 0:pad, lanes:lanes + BLK] = high
                dest[at, pad:2 * pad, lanes:lanes + BLK] = low
        return carry

    sends = {}
    for bit in range(dom_bits):
        moves = [d for d in range(doms) if d % (1 << bit) == 0 and (d >> bit) & 1]
        for d in sorted(moves, reverse=True):
            to = d ^ (1 << bit)
            for c in range(nchunk):
                at = pl.ds(c * chunk, chunk)
                sends[(bit, d, c)] = pltpu.make_async_remote_copy(
                    src_ref=(mine if bit == 0 else passed).at[d, at],
                    dst_ref=got.at[bit, to, at],
                    send_sem=tab_send.at[bit, d, c],
                    recv_sem=tab_recv.at[bit, to, c],
                    device_id={"dom": me ^ (1 << bit)},
                    device_id_type=MESH,
                )

    def forward(bit, d):
        for c in range(nchunk):
            at = pl.ds(c * chunk, chunk)
            total = mine[d, at]
            for earlier in range(bit):
                sends[(earlier, d | (1 << earlier), c)].wait_recv()
                total = total + got[earlier, d, at]
            passed[d, at] = total
            sends[(bit, d, c)].start()

    for d in reversed(range(doms)):
        if d & 1 and d > 1:
            for c in range(nchunk):
                gather(d, c)
                sends[(0, d, c)].start()
    for d in reversed(range(2, doms)):
        if not d & 1:
            gather(d)
    for bit in range(1, dom_bits):
        for d in reversed(range(doms)):
            if d % (1 << bit) == 0 and (d >> bit) & 1:
                forward(bit, d)
    for c in range(nchunk):
        gather(1, c)
        sends[(0, 1, c)].start()
    gather(0)
    loads[2].wait()
    loads[3].wait()
    lax.fori_loop(0, nblk, convert, 0)

    acc[...] = jnp.zeros(acc.shape, F32)
    lane = lax.broadcasted_iota(jnp.int32, (2 * branches, BLK), 1)
    times = [lengths_s[chosen_s[b]] for b in range(branches)]

    def block(n, carry):
        tile = mine[0, n]
        for bit in range(dom_bits):
            tile = tile + got[bit, 0, n]
        turned = jnp.transpose(tile)
        w_row = tile[states + 1:states + 2, pad:2 * pad]
        l_high, l_low = split(turned[0:pad, :] * w_row)
        r_high, r_low = split(tile[:, pad:2 * pad])
        l_all = jnp.concatenate([l_high, l_high, l_low], axis=1)
        r_all = jnp.concatenate([r_high, r_high, r_low], axis=1)
        expo = jnp.broadcast_to(turned[pad:2 * pad, states:states + 1], (pad, BLK))
        for half in range(branches // 2):
            at = n * (branches // 2) + half
            t_x = top_x[at]
            b_x = bottom_x[at]
            lefts = jnp.dot(
                l_all, jnp.concatenate([t_x, t_x[0:pad]], axis=0), preferred_element_type=F32
            )
            rights = jnp.dot(
                r_all, jnp.concatenate([b_x, b_x[0:pad]], axis=0), preferred_element_type=F32
            )
            joint = lefts * rights
            for side in range(2):
                b = 2 * half + side
                decayed = joint[:, side * BLK:(side + 1) * BLK] * jnp.exp(expo * times[b])
                once = decayed * expo
                twice = once * expo
                like_v[0, b:b + 1, :] = jnp.sum(decayed, axis=0, keepdims=True)
                like_v[1, b:b + 1, :] = jnp.sum(once, axis=0, keepdims=True)
                like_v[2, b:b + 1, :] = jnp.sum(twice, axis=0, keepdims=True)
        like0 = like_v[0]
        first_d = like_v[1] / like0
        second_d = like_v[2] / like0 - first_d * first_d
        w_sites = pattern_ref[pl.ds(n, 1), :].astype(F32)
        like_ref[pl.ds(n, branches, stride=nblk), :] = like0
        both = jnp.concatenate([first_d, second_d], axis=0) * w_sites
        sums = jnp.sum(both, axis=1, keepdims=True)
        p = blocks_s[0, n]
        for d in range(doms):
            hit = jnp.logical_and(lane + d * owned == p, lane < owned)
            hit = jnp.logical_or(hit, lane == owned)
            acc[d] = acc[d] + jnp.where(hit, sums, 0.0)
        return carry

    for c in range(nchunk):
        for bit in range(dom_bits):
            sends[(bit, 1 << bit, c)].wait_recv()
        lax.fori_loop(c * chunk, (c + 1) * chunk, block, 0)

    scatter = []
    for d, x in reversed(plane):
        copy = pltpu.make_async_remote_copy(
            src_ref=acc.at[me ^ d],
            dst_ref=dom_in.at[me * inner + near],
            send_sem=dom_send.at[d * inner + x],
            recv_sem=dom_recv.at[d * inner + x],
            device_id=in_plane(d, x),
            device_id_type=MESH,
        )
        copy.start()
        scatter.append(copy)
    dom_in[me * inner + near] = acc[me]
    for copy in scatter:
        copy.wait_recv()
    total = dom_in[0]
    for d in range(1, doms * inner):
        total = total + dom_in[d]
    site_out[...] = total
    spread = []
    for k in range(1, outer):
        copy = pltpu.make_async_remote_copy(
            src_ref=site_out,
            dst_ref=site_in.at[far],
            send_sem=site_send.at[k],
            recv_sem=site_recv.at[k],
            device_id=in_line(k),
            device_id_type=MESH,
        )
        copy.start()
        spread.append(copy)
    site_in[far] = total
    for copy in spread:
        copy.wait_recv()
    total = site_in[0]
    for z in range(1, outer):
        total = total + site_in[z]

    sums = total[:, owned:owned + 1]
    ratio = sums[0:branches] / sums[branches:2 * branches]
    row = lax.broadcasted_iota(jnp.int32, (branches, BLK), 0)
    old = jnp.zeros((branches, BLK), F32)
    for b in range(branches):
        old = jnp.where(row == b, times[b], old)
    final_ref[0:2 * branches, :] = total
    final_ref[2 * branches:3 * branches, :] = old - ratio

    for copy in scatter + spread:
        copy.wait_send()
    for copy in sends.values():
        copy.wait_send()


def write(
    cfg, like_ref, final_ref, pattern_ref, chosen_s, lengths_ref, loglik_ref, share_ref, new_ref
):
    branches, nblk, owned = cfg
    weights = pattern_ref[...].astype(F32)
    for b in range(branches):
        rows = pl.ds(b * nblk, nblk)
        loglik_ref[rows, :] = weights * jnp.log(like_ref[rows, :])
    share_ref[...] = final_ref[0:2 * branches, 0:owned]
    new = lengths_ref[...]
    place = lax.broadcasted_iota(jnp.int32, new.shape, 1)
    for b in range(branches):
        value = final_ref[2 * branches + b:2 * branches + b + 1, 0:1]
        new = jnp.where(place == chosen_s[b], value, new)
    new_ref[...] = new


def on_device(
    top_partial,
    bottom_partial,
    left_vectors,
    right_vectors,
    decay_rates,
    state_weights,
    part_rates,
    branch_lengths,
    pattern_weights,
    block_partition,
    chosen_branches,
):
    doms = lax.axis_size("dom")
    sites = lax.axis_size("site")
    branches, states, _, sites_here = top_partial.shape
    nblk = sites_here // BLK
    owned = left_vectors.shape[0]
    tree = branch_lengths.shape[0]
    pad = round_up(states + 2, 64)
    chunk = 2 if nblk % 2 == 0 else 1
    nchunk = nblk // chunk
    dom_bits = doms.bit_length() - 1
    inner = 2 if sites % 2 == 0 else 1
    outer = sites // inner
    used = branches * states * nblk
    room = used + (pad - states) * nblk
    cfg = (doms, sites, inner, branches, states, nblk, owned, pad, chunk)
    hbm = pl.BlockSpec(memory_space=pl.ANY)
    vmem = pl.BlockSpec(memory_space=pltpu.VMEM)
    smem = pl.BlockSpec(memory_space=pltpu.SMEM)
    tile = (pad, 2 * pad)
    dma = pltpu.SemaphoreType.DMA
    pattern = pattern_weights.reshape(nblk, BLK)
    like, final = pl.pallas_call(
        functools.partial(body, cfg),
        out_shape=(
            jax.ShapeDtypeStruct((branches * nblk, BLK), F32),
            jax.ShapeDtypeStruct((3 * branches, BLK), F32),
        ),
        in_specs=[hbm, hbm, hbm, hbm, vmem, vmem, smem, smem, smem, vmem, smem, vmem],
        out_specs=(vmem, vmem),
        scratch_shapes=[
            pltpu.VMEM((room, BLK), F32),
            pltpu.VMEM((room, BLK), F32),
            pltpu.VMEM((states * owned, states), F32),
            pltpu.VMEM((states * owned, states), F32),
            pltpu.VMEM((doms, 1, BLK), jnp.int32),
            pltpu.SMEM((doms, 1, BLK), jnp.int32),
            pltpu.VMEM((doms, nblk) + tile, F32),
            pltpu.VMEM((doms, nblk) + tile, F32),
            pltpu.VMEM((dom_bits, doms, nblk) + tile, F32),
            pltpu.VMEM((nblk * branches // 2, 2 * pad, 2 * BLK), BF16),
            pltpu.VMEM((nblk * branches // 2, 2 * pad, 2 * BLK), BF16),
            pltpu.VMEM((3, branches, BLK), F32),
            pltpu.VMEM((doms, 2 * branches, BLK), F32),
            pltpu.VMEM((doms * inner, 2 * branches, BLK), F32),
            pltpu.VMEM((2 * branches, BLK), F32),
            pltpu.VMEM((outer, 2 * branches, BLK), F32),
            dma((4,)),
            dma((doms,)),
            dma((doms,)),
            dma,
            dma((dom_bits, doms, nchunk)),
            dma((dom_bits, doms, nchunk)),
            dma((doms * inner,)),
            dma((doms * inner,)),
            dma((outer,)),
            dma((outer,)),
        ],
        compiler_params=pltpu.CompilerParams(
            collective_id=0, has_side_effects=True, vmem_limit_bytes=56 * 1024 * 1024
        ),
    )(
        top_partial.reshape(used, BLK),
        bottom_partial.reshape(used, BLK),
        jnp.swapaxes(left_vectors, 0, 1).reshape(states * owned, states),
        jnp.swapaxes(right_vectors, 0, 1).reshape(states * owned, states),
        decay_rates,
        state_weights,
        part_rates,
        branch_lengths,
        chosen_branches,
        pattern,
        block_partition,
        block_partition,
    )
    loglik, share, new = pl.pallas_call(
        functools.partial(write, (branches, nblk, owned)),
        out_shape=(
            jax.ShapeDtypeStruct((branches * nblk, BLK), F32),
            jax.ShapeDtypeStruct((2 * branches, owned), F32),
            jax.ShapeDtypeStruct((1, tree), F32),
        ),
        in_specs=[vmem, vmem, vmem, smem, vmem],
        out_specs=(vmem, vmem, vmem),
    )(like, final, pattern, chosen_branches, branch_lengths.reshape(1, tree))
    return (
        loglik.reshape(branches, 1, sites_here),
        share.reshape(2, branches, owned),
        new.reshape(tree),
    )


def solution(mesh):
    return jax.shard_map(
        on_device,
        mesh=mesh,
        in_specs=(
            P(None, None, "dom", "site"),
            P(None, None, "dom", "site"),
            P("dom", None, None),
            P("dom", None, None),
            P("dom", None),
            P("dom", None),
            P("dom"),
            P(),
            P("dom", "site"),
            P("dom", "site"),
            P(),
        ),
        out_specs=(P(None, "dom", "site"), P(None, None, "dom"), P()),
        check_vma=False,
    )
```

```python
import functools

import jax
import jax.numpy as jnp
from jax import lax
from jax.experimental import pallas as pl
from jax.experimental.pallas import tpu as pltpu
from jax.sharding import PartitionSpec as P

BLK = 128
MESH = pl.DeviceIdType.MESH
F32 = jnp.float32
BF16 = jnp.bfloat16


def round_up(value, unit):
    return (value + unit - 1) // unit * unit


def split(value):
    high = value.astype(BF16)
    return high, (value - high.astype(F32)).astype(BF16)


def body(
    cfg,
    top_hbm, bottom_hbm, left_hbm, right_hbm,
    decay_hbm, weight_hbm, rate_hbm, lengths_hbm, chosen_hbm,
    pattern_hbm, blocks_hbm,
    like_ref, final_ref,
    top_v, bottom_v, left_v, right_v, req_v, req_s, mine, passed, got,
    top_x, bottom_x, like_v, acc, dom_in, site_out, site_in,
    decay_ref, weight_ref, rate_s, lengths_s, chosen_s, pattern_ref, blocks_s, blocks_ref,
    load_sem, small_sem, req_send, req_recv, req_local, tab_send, tab_recv,
    dom_send, dom_recv, site_send, site_recv,
):
    doms, sites, inner, branches, states, nblk, owned, pad, chunk = cfg
    me = lax.axis_index("dom")
    spot = lax.axis_index("site")
    dom_bits = doms.bit_length() - 1
    outer = sites // inner
    near, far = lax.rem(spot, inner), spot // inner
    nchunk = nblk // chunk
    used = branches * states * nblk

    plane = [(d, x) for d in range(doms) for x in range(inner) if d or x]

    def in_plane(d, x):
        return {"dom": me ^ d, "site": far * inner + lax.rem(near + x, inner)}

    def in_line(k):
        return {"site": lax.rem(far + k, outer) * inner + near}

    loads = [
        pltpu.make_async_copy(left_hbm, left_v, load_sem.at[0]),
        pltpu.make_async_copy(right_hbm, right_v, load_sem.at[1]),
        pltpu.make_async_copy(top_hbm, top_v.at[pl.ds(0, used)], load_sem.at[2]),
        pltpu.make_async_copy(bottom_hbm, bottom_v.at[pl.ds(0, used)], load_sem.at[3]),
    ]
    small = [
        pltpu.make_async_copy(source, dest, small_sem.at[i])
        for i, (source, dest) in enumerate((
            (blocks_hbm, blocks_ref),
            (decay_hbm, decay_ref),
            (weight_hbm, weight_ref),
            (rate_hbm, rate_s),
            (blocks_hbm, blocks_s),
            (lengths_hbm, lengths_s),
            (chosen_hbm, chosen_s),
            (pattern_hbm, pattern_ref),
        ))
    ]

    barrier = pltpu.get_barrier_semaphore()
    for d, x in plane:
        pl.semaphore_signal(barrier, inc=1, device_id=in_plane(d, x), device_id_type=MESH)
    for k in range(1, outer):
        pl.semaphore_signal(barrier, inc=1, device_id=in_line(k), device_id_type=MESH)

    for load in small + loads[:2]:
        load.start()
    req_v[0] = jnp.zeros((1, BLK), jnp.int32)
    tail = top_v.shape[0] - used
    top_v[pl.ds(used, tail), :] = jnp.zeros((tail, BLK), F32)
    bottom_v[pl.ds(used, tail), :] = jnp.zeros((tail, BLK), F32)
    mine[...] = jnp.zeros(mine.shape, F32)

    small[0].wait()
    req_v[0, 0:1, 0:nblk] = blocks_ref[...]
    pl.semaphore_wait(barrier, len(plane) + outer - 1)

    asks = []
    for delta in range(1, doms):
        ask = pltpu.make_async_remote_copy(
            src_ref=req_v.at[0],
            dst_ref=req_v.at[delta],
            send_sem=req_send.at[delta],
            recv_sem=req_recv.at[delta],
            device_id={"dom": me ^ delta},
            device_id_type=MESH,
        )
        ask.start()
        asks.append(ask)
    for load in small[1:] + loads[:2]:
        load.wait()
    loads[2].start()
    loads[3].start()
    for ask in asks:
        ask.wait()
    local = pltpu.make_async_copy(req_v, req_s, req_local)
    local.start()
    local.wait()

    def gather(delta, c=None):
        def step(n, carry):
            relative = req_s[delta, 0, n] - me * owned
            inside = jnp.logical_and(relative >= 0, relative < owned)
            keep = jnp.where(inside, 1.0, 0.0).astype(F32)
            p = jnp.clip(relative, 0, owned - 1)
            mine[delta, n, 0:states, 0:states] = left_v[pl.ds(p, states, stride=owned), :] * keep
            mine[delta, n, 0:states, pad:pad + states] = right_v[pl.ds(p, states, stride=owned), :] * keep
            rate = rate_s[p] * keep
            mine[delta, n, states:states + 1, pad:pad + states] = -decay_ref[pl.ds(p, 1), :] * rate
            mine[delta, n, states + 1:states + 2, pad:pad + states] = (
                weight_ref[pl.ds(p, 1), :] * keep
            )
            return carry

        if c is None:
            lax.fori_loop(0, nblk, step, 0)
        else:
            lax.fori_loop(c * chunk, (c + 1) * chunk, step, 0, unroll=True)

    def convert(n, carry):
        for source, dest in ((top_v, top_x), (bottom_v, bottom_x)):
            for b in range(branches):
                rows = source[pl.ds(b * states * nblk + n, pad, stride=nblk), :]
                high, low = split(rows)
                at = n * (branches // 2) + b // 2
                lanes = (b % 2) * BLK
                dest[at, 0:pad, lanes:lanes + BLK] = high
                dest[at, pad:2 * pad, lanes:lanes + BLK] = low
        return carry

    sends = {}
    for bit in range(dom_bits):
        moves = [d for d in range(doms) if d % (1 << bit) == 0 and (d >> bit) & 1]
        for d in sorted(moves, reverse=True):
            to = d ^ (1 << bit)
            for c in range(nchunk):
                at = pl.ds(c * chunk, chunk)
                sends[(bit, d, c)] = pltpu.make_async_remote_copy(
                    src_ref=(mine if bit == 0 else passed).at[d, at],
                    dst_ref=got.at[bit, to, at],
                    send_sem=tab_send.at[bit, d, c],
                    recv_sem=tab_recv.at[bit, to, c],
                    device_id={"dom": me ^ (1 << bit)},
                    device_id_type=MESH,
                )

    def forward(bit, d):
        for c in range(nchunk):
            at = pl.ds(c * chunk, chunk)
            total = mine[d, at]
            for earlier in range(bit):
                sends[(earlier, d | (1 << earlier), c)].wait_recv()
                total = total + got[earlier, d, at]
            passed[d, at] = total
            sends[(bit, d, c)].start()

    for d in reversed(range(doms)):
        if d & 1 and d > 1:
            for c in range(nchunk):
                gather(d, c)
                sends[(0, d, c)].start()
    for d in reversed(range(2, doms)):
        if not d & 1:
            gather(d)
    for bit in range(1, dom_bits):
        for d in reversed(range(doms)):
            if d % (1 << bit) == 0 and (d >> bit) & 1:
                forward(bit, d)
    for c in range(nchunk):
        gather(1, c)
        sends[(0, 1, c)].start()
    gather(0)
    loads[2].wait()
    loads[3].wait()
    lax.fori_loop(0, nblk, convert, 0)

    acc[...] = jnp.zeros(acc.shape, F32)
    lane = lax.broadcasted_iota(jnp.int32, (2 * branches, BLK), 1)
    times = [lengths_s[chosen_s[b]] for b in range(branches)]

    def block(n, carry):
        tile = mine[0, n]
        for bit in range(dom_bits):
            tile = tile + got[bit, 0, n]
        turned = jnp.transpose(tile)
        w_row = tile[states + 1:states + 2, pad:2 * pad]
        l_high, l_low = split(turned[0:pad, :] * w_row)
        r_high, r_low = split(tile[:, pad:2 * pad])
        l_all = jnp.concatenate([l_high, l_high, l_low], axis=1)
        r_all = jnp.concatenate([r_high, r_high, r_low], axis=1)
        expo = jnp.broadcast_to(turned[pad:2 * pad, states:states + 1], (pad, BLK))
        for half in range(branches // 2):
            at = n * (branches // 2) + half
            t_x = top_x[at]
            b_x = bottom_x[at]
            lefts = jnp.dot(
                l_all, jnp.concatenate([t_x, t_x[0:pad]], axis=0), preferred_element_type=F32
            )
            rights = jnp.dot(
                r_all, jnp.concatenate([b_x, b_x[0:pad]], axis=0), preferred_element_type=F32
            )
            joint = lefts * rights
            for side in range(2):
                b = 2 * half + side
                decayed = joint[:, side * BLK:(side + 1) * BLK] * jnp.exp(expo * times[b])
                once = decayed * expo
                twice = once * expo
                like_v[0, b:b + 1, :] = jnp.sum(decayed, axis=0, keepdims=True)
                like_v[1, b:b + 1, :] = jnp.sum(once, axis=0, keepdims=True)
                like_v[2, b:b + 1, :] = jnp.sum(twice, axis=0, keepdims=True)
        like0 = like_v[0]
        first_d = like_v[1] / like0
        second_d = like_v[2] / like0 - first_d * first_d
        w_sites = pattern_ref[pl.ds(n, 1), :].astype(F32)
        like_ref[pl.ds(n, branches, stride=nblk), :] = like0
        both = jnp.concatenate([first_d, second_d], axis=0) * w_sites
        sums = jnp.sum(both, axis=1, keepdims=True)
        p = blocks_s[0, n]
        for d in range(doms):
            hit = jnp.logical_and(lane + d * owned == p, lane < owned)
            hit = jnp.logical_or(hit, lane == owned)
            acc[d] = acc[d] + jnp.where(hit, sums, 0.0)
        return carry

    for c in range(nchunk):
        for bit in range(dom_bits):
            sends[(bit, 1 << bit, c)].wait_recv()
        lax.fori_loop(c * chunk, (c + 1) * chunk, block, 0, unroll=True)

    scatter = []
    for d, x in reversed(plane):
        copy = pltpu.make_async_remote_copy(
            src_ref=acc.at[me ^ d],
            dst_ref=dom_in.at[me * inner + near],
            send_sem=dom_send.at[d * inner + x],
            recv_sem=dom_recv.at[d * inner + x],
            device_id=in_plane(d, x),
            device_id_type=MESH,
        )
        copy.start()
        scatter.append(copy)
    dom_in[me * inner + near] = acc[me]
    for copy in scatter:
        copy.wait_recv()
    total = dom_in[0]
    for d in range(1, doms * inner):
        total = total + dom_in[d]
    site_out[...] = total
    spread = []
    for k in range(1, outer):
        copy = pltpu.make_async_remote_copy(
            src_ref=site_out,
            dst_ref=site_in.at[far],
            send_sem=site_send.at[k],
            recv_sem=site_recv.at[k],
            device_id=in_line(k),
            device_id_type=MESH,
        )
        copy.start()
        spread.append(copy)
    site_in[far] = total
    for copy in spread:
        copy.wait_recv()
    total = site_in[0]
    for z in range(1, outer):
        total = total + site_in[z]

    sums = total[:, owned:owned + 1]
    ratio = sums[0:branches] / sums[branches:2 * branches]
    row = lax.broadcasted_iota(jnp.int32, (branches, BLK), 0)
    old = jnp.zeros((branches, BLK), F32)
    for b in range(branches):
        old = jnp.where(row == b, times[b], old)
    final_ref[0:2 * branches, :] = total
    final_ref[2 * branches:3 * branches, :] = old - ratio

    for copy in scatter + spread:
        copy.wait_send()
    for copy in sends.values():
        copy.wait_send()


def write(
    cfg, like_ref, final_ref, pattern_ref, chosen_s, lengths_ref, loglik_ref, share_ref, new_ref
):
    branches, nblk, owned = cfg
    weights = pattern_ref[...].astype(F32)
    for b in range(branches):
        rows = pl.ds(b * nblk, nblk)
        loglik_ref[rows, :] = weights * jnp.log(like_ref[rows, :])
    share_ref[...] = final_ref[0:2 * branches, 0:owned]
    new = lengths_ref[...]
    place = lax.broadcasted_iota(jnp.int32, new.shape, 1)
    for b in range(branches):
        value = final_ref[2 * branches + b:2 * branches + b + 1, 0:1]
        new = jnp.where(place == chosen_s[b], value, new)
    new_ref[...] = new


def on_device(
    top_partial,
    bottom_partial,
    left_vectors,
    right_vectors,
    decay_rates,
    state_weights,
    part_rates,
    branch_lengths,
    pattern_weights,
    block_partition,
    chosen_branches,
):
    doms = lax.axis_size("dom")
    sites = lax.axis_size("site")
    branches, states, _, sites_here = top_partial.shape
    nblk = sites_here // BLK
    owned = left_vectors.shape[0]
    tree = branch_lengths.shape[0]
    pad = round_up(states + 2, 64)
    chunk = 2 if nblk % 2 == 0 else 1
    nchunk = nblk // chunk
    dom_bits = doms.bit_length() - 1
    inner = 2 if sites % 2 == 0 else 1
    outer = sites // inner
    used = branches * states * nblk
    room = used + (pad - states) * nblk
    cfg = (doms, sites, inner, branches, states, nblk, owned, pad, chunk)
    hbm = pl.BlockSpec(memory_space=pl.ANY)
    vmem = pl.BlockSpec(memory_space=pltpu.VMEM)
    smem = pl.BlockSpec(memory_space=pltpu.SMEM)
    tile = (pad, 2 * pad)
    dma = pltpu.SemaphoreType.DMA
    pattern = pattern_weights.reshape(nblk, BLK)
    like, final = pl.pallas_call(
        functools.partial(body, cfg),
        out_shape=(
            jax.ShapeDtypeStruct((branches * nblk, BLK), F32),
            jax.ShapeDtypeStruct((3 * branches, BLK), F32),
        ),
        in_specs=[hbm] * 11,
        out_specs=(vmem, vmem),
        scratch_shapes=[
            pltpu.VMEM((room, BLK), F32),
            pltpu.VMEM((room, BLK), F32),
            pltpu.VMEM((states * owned, states), F32),
            pltpu.VMEM((states * owned, states), F32),
            pltpu.VMEM((doms, 1, BLK), jnp.int32),
            pltpu.SMEM((doms, 1, BLK), jnp.int32),
            pltpu.VMEM((doms, nblk) + tile, F32),
            pltpu.VMEM((doms, nblk) + tile, F32),
            pltpu.VMEM((dom_bits, doms, nblk) + tile, F32),
            pltpu.VMEM((nblk * branches // 2, 2 * pad, 2 * BLK), BF16),
            pltpu.VMEM((nblk * branches // 2, 2 * pad, 2 * BLK), BF16),
            pltpu.VMEM((3, branches, BLK), F32),
            pltpu.VMEM((doms, 2 * branches, BLK), F32),
            pltpu.VMEM((doms * inner, 2 * branches, BLK), F32),
            pltpu.VMEM((2 * branches, BLK), F32),
            pltpu.VMEM((outer, 2 * branches, BLK), F32),
            pltpu.VMEM((owned, states), F32),
            pltpu.VMEM((owned, states), F32),
            pltpu.SMEM((owned,), F32),
            pltpu.SMEM((tree,), F32),
            pltpu.SMEM((branches,), jnp.int32),
            pltpu.VMEM((nblk, BLK), jnp.int32),
            pltpu.SMEM((1, nblk), jnp.int32),
            pltpu.VMEM((1, nblk), jnp.int32),
            dma((4,)),
            dma((8,)),
            dma((doms,)),
            dma((doms,)),
            dma,
            dma((dom_bits, doms, nchunk)),
            dma((dom_bits, doms, nchunk)),
            dma((doms * inner,)),
            dma((doms * inner,)),
            dma((outer,)),
            dma((outer,)),
        ],
        compiler_params=pltpu.CompilerParams(
            collective_id=0, has_side_effects=True, vmem_limit_bytes=56 * 1024 * 1024
        ),
    )(
        top_partial.reshape(used, BLK),
        bottom_partial.reshape(used, BLK),
        jnp.swapaxes(left_vectors, 0, 1).reshape(states * owned, states),
        jnp.swapaxes(right_vectors, 0, 1).reshape(states * owned, states),
        decay_rates,
        state_weights,
        part_rates,
        branch_lengths,
        chosen_branches,
        pattern,
        block_partition,
    )
    loglik, share, new = pl.pallas_call(
        functools.partial(write, (branches, nblk, owned)),
        out_shape=(
            jax.ShapeDtypeStruct((branches * nblk, BLK), F32),
            jax.ShapeDtypeStruct((2 * branches, owned), F32),
            jax.ShapeDtypeStruct((1, tree), F32),
        ),
        in_specs=[vmem, vmem, vmem, smem, vmem],
        out_specs=(vmem, vmem, vmem),
    )(like, final, pattern, chosen_branches, branch_lengths.reshape(1, tree))
    return (
        loglik.reshape(branches, 1, sites_here),
        share.reshape(2, branches, owned),
        new.reshape(tree),
    )


def solution(mesh):
    return jax.shard_map(
        on_device,
        mesh=mesh,
        in_specs=(
            P(None, None, "dom", "site"),
            P(None, None, "dom", "site"),
            P("dom", None, None),
            P("dom", None, None),
            P("dom", None),
            P("dom", None),
            P("dom"),
            P(),
            P("dom", "site"),
            P("dom", "site"),
            P(),
        ),
        out_specs=(P(None, "dom", "site"), P(None, None, "dom"), P()),
        check_vma=False,
    )
```
